32 devices in a mesh: gx: 4 (over x, core), gy: 8 (over z, y).
Axes of the slice: x: 2, y: 2, z: 4, core: 2. Of those that a mesh axis runs over, the one named last changes fastest.
Arguments:
- velocity: float32 [3, 1024, 512], P(None, ('gx', 'gy')), may hold values from -6 to 6
- depart: float32 [3, 524288], P(None, ('gx', 'gy')), may hold values from -1 to 1
- owner_rank: int32 [524288, 1], P(('gx', 'gy')), may hold values from 0 to 31; in each aligned block of 16384 rows (0 to 16383, 16384 to 32767, ...) at most 1024 rows name the same one
- owner_element_index: int32 [524288], P(('gx', 'gy')), may hold values from 0 to 31
- neighbours: int32 [6, 1024], P(None, ('gx', 'gy')), may hold values from -1 to 1023, as said below
Outputs:
- advected: float32 [3, 1024, 512], P(None, ('gx', 'gy'))
The draws below stay inside these ranges and needn't reach their ends.
Inputs may be any that keep to these rules, and one draw needn't show every extreme that they name: `owner_rank`: within the rows of one device no owner device is named by more than 1024 rows, and in some device's rows one owner is named exactly 1024 times. `neighbours`: -1 marks a boundary face; any other entry is an element of the same block of 32 consecutive elements as the entry's own element, or of the block just before or just after it.
All inputs are finite; a program needn't handle non-finite values.
Results may differ from the reference program's by a relative error of at most 0.0003.
Values sent between devices are 32-bit elements; how exact they have to be, the bound alone decides.
No kernel may reach another device: no remote copies, remote signals or barrier semaphores. Data moves between devices by JAX's collectives and lax.ppermute only.
A program may use at most 64 MiB of HBM per device.

```python
import math
import jax
import jax.numpy as jnp
import numpy as np
from jax import lax

VELOCITY_PARTS = 3
NODES = 512
E_DEV = 32
ELEMS = 1024
POINTS = 524288
CAP = 1024
DEVICES = 32


def draw_neighbours(key, part):
    elem_total = ELEMS
    element = jnp.arange(elem_total, dtype=jnp.int32)
    block_of = element // E_DEV
    lowest = jnp.maximum(block_of - 1, 0) * E_DEV
    highest = jnp.minimum(block_of + 2, elem_total // E_DEV) * E_DEV
    pick_key, edge_key = jax.random.split(key)
    offset = jax.random.randint(pick_key, (6, elem_total), 0, 1 << 30, dtype=jnp.int32) % (highest - lowest)[None, :]
    picked = lowest[None, :] + offset
    boundary = jax.random.randint(edge_key, (6, elem_total), 0, 6, dtype=jnp.int32)
    return jnp.where(boundary == 0, -1, picked).astype(jnp.int32)


def place_ends(drawn, rng, least, high):
    spot = [jax.random.randint(jax.random.fold_in(rng, axis), (), 0, length) for axis, length in enumerate(drawn.shape)]
    widest = drawn.shape.index(max(drawn.shape))
    beside = spot[:widest] + [(spot[widest] + 1) % drawn.shape[widest]] + spot[widest + 1:]
    return drawn.at[tuple(spot)].set(least).at[tuple(beside)].set(high)


def shard_levels(rng, shape, shards, smallest, largest):
    level = 1.0
    for axis_at, parts in shards:
        steps = jax.random.uniform(jax.random.fold_in(jax.random.fold_in(rng, 6), axis_at), (parts,), jnp.float32, smallest / len(shards), largest / len(shards))
        level = level * jnp.repeat(jnp.exp(steps), shape[axis_at] // parts).reshape((-1,) + (1,) * (len(shape) - 1 - axis_at))
    return level


def shared_out(rng, own, number, rows, number_of, top, reach, skew):
    ranking = jax.random.permutation(rng, number_of)
    crowded, ordinary = portions_of(number_of, rows * top, reach, skew, True), portions_of(number_of, rows * top, reach, skew, False)
    places = jnp.arange(number_of)

    def named(lengths, turn):
        used = int((lengths > 0).sum())
        fixed = max(1, used // 4)
        moved = fixed + (places - fixed + turn * (used - fixed)) % max(1, number_of - fixed)
        return jnp.zeros((number_of,), jnp.int32).at[ranking[jnp.where(places < fixed, places, moved)]].set(jnp.asarray(lengths, jnp.int32))

    lengths = jnp.where(number % 4 == 0, named(crowded, number // 4), named(ordinary, number - number // 4 - 1))
    mixed = jax.random.permutation(jax.random.fold_in(own, 3), number_of)
    source_of, receiver = mixed[0:number_of // 2 * 2:2], mixed[1:number_of // 2 * 2:2]
    room = jnp.minimum(lengths[source_of] - 1, reach - lengths[receiver]) // 2
    room = jnp.where((source_of == ranking[0]) | (receiver == ranking[0]) | (lengths[receiver] == 0), 0, jnp.maximum(room, 0))
    moved = jax.random.randint(jax.random.fold_in(own, 4), (number_of // 2,), 0, 1 << 20) % (room + 1)
    lengths = lengths.at[source_of].add(-moved).at[receiver].add(moved)
    members = jnp.searchsorted(jnp.cumsum(lengths), jnp.arange(rows * top), side="right").astype(jnp.int32)
    listing = members.reshape(top, rows).T
    listing = listing[jax.random.permutation(jax.random.fold_in(own, 1), rows)]
    turn = jax.random.randint(jax.random.fold_in(own, 2), (rows, 1), 0, top)
    return jnp.take_along_axis(listing, (jnp.arange(top)[None, :] + turn) % top, axis=1)


def portions_of(amount, total, most, lean, full):
    weights = [(1 << 20) // math.isqrt(standing ** lean) + 1 for standing in range(1, amount + 1)]
    largest = most if full else min(most, max(-(-total // amount), total * weights[0] // sum(weights)))
    least = 1 if total - largest >= amount - 1 else 0
    counts, surplus = [largest] + [least] * (amount - 1), total - largest - least * (amount - 1)
    while surplus > 0:
        candidates = [i for i in range(1, amount) if counts[i] < largest] or [i for i in range(1, amount) if counts[i] < most]
        whole, left = sum([weights[i] for i in candidates]), surplus
        for i in candidates:
            extra = min(most - counts[i], max(1, left * weights[i] // whole), surplus)
            counts[i] = counts[i] + extra
            surplus = surplus - extra
    return np.array(counts)


def gaussian(stream_key, extent, scale, limit, cuts=(), kind=jnp.bfloat16):
    values = jax.random.normal(stream_key, extent, jnp.float32) * scale
    if len(cuts) > 0:
        values = shard_levels(stream_key, extent, cuts, -0.22, 0.18) * values
    return jnp.clip(values, min=-limit, max=limit).astype(kind)


def setup_inputs(seed: int = 0) -> dict:
    splits = jax.random.split(jax.random.key(seed), 6)
    velocity = gaussian(splits[0], (VELOCITY_PARTS, ELEMS, NODES), 1.0, 6.0, ((1, 32),), jnp.float32)
    depart = jnp.clip(jax.random.uniform(splits[1], (VELOCITY_PARTS, POINTS), jnp.float32, -1.0, 1.0) * shard_levels(splits[1], (VELOCITY_PARTS, POINTS), ((1, 32),), -0.4, 0.0), -1.0, 1.0)
    owner_rank_keys = jax.random.split(jax.random.fold_in(splits[2], 1), POINTS // (E_DEV * NODES))
    owner_rank_turns = jax.random.permutation(jax.random.fold_in(splits[2], 3), POINTS // (E_DEV * NODES))
    owner_rank = jax.vmap(lambda own, number: shared_out(jax.random.fold_in(splits[2], 2), own, number, E_DEV * NODES, DEVICES, 1, CAP, 2))(owner_rank_keys, owner_rank_turns).reshape((POINTS, 1))
    owner_element_index = place_ends(jax.random.randint(splits[3], (POINTS,), 0, E_DEV), jax.random.fold_in(splits[3], 1), 0, E_DEV - 1).astype(jnp.int32)
    neighbours = draw_neighbours(jax.random.fold_in(splits[5], 71), 0)
    return {"velocity": velocity, "depart": depart, "owner_rank": owner_rank, "owner_element_index": owner_element_index, "neighbours": neighbours}


GLL_POINTS = np.array([-1.0, -0.8717401485096066, -0.5917001814331423, -0.2092992179024789, 0.2092992179024789, 0.5917001814331423, 0.8717401485096066, 1.0])


def lagrange(coords):
    columns = []
    for node_id in range(8):
        factor = jnp.ones_like(coords)
        for other in range(8):
            if other != node_id:
                factor = factor * ((coords - float(GLL_POINTS[other])) / float(GLL_POINTS[node_id] - GLL_POINTS[other]))
        columns.append(factor)
    return jnp.stack(columns, axis=-1)


def face_slicer(face_id):
    whole_range = slice(None)
    edge_at = 7 * (face_id % 2)
    if face_id < 2:
        return (whole_range, whole_range, edge_at)
    if face_id < 4:
        return (whole_range, whole_range, whole_range, edge_at)
    return (whole_range, whole_range, whole_range, whole_range, edge_at)


def faces_of(nodal_cube):
    shape_lead = (nodal_cube.shape[0], nodal_cube.shape[1], 64)
    return jnp.stack([nodal_cube[face_slicer(face_id)].reshape(shape_lead) for face_id in range(6)], axis=1)


def apply_faces(nodal_cube, own_faces, neighbour_faces, local_index, present):
    result = nodal_cube
    for face_id in range(6):
        across_elements = neighbour_faces[:, face_id ^ 1][:, local_index[face_id]]
        change = jnp.where(present[face_id][None, :, None], 0.5 * (across_elements - own_faces[:, face_id]), 0.0)
        result = result.at[face_slicer(face_id)].add(change.reshape(result.shape[0], result.shape[1], 8, 8))
    return result


def reference(velocity, depart, owner_rank, owner_element_index, neighbours):
    owners = (owner_rank[:, 0] * E_DEV + owner_element_index).astype(jnp.int32)
    block_count = POINTS // 4096
    coord_blocks = depart.reshape(3, block_count, 4096).transpose(1, 0, 2)
    owner_blocks = owners.reshape(block_count, 4096)

    def one_block(block_pair):
        coords, owner_row_table = block_pair
        weights = lagrange(coords)
        gathered = jnp.take(velocity, owner_row_table, axis=1).reshape(3, 4096, 8, 8, 8)
        along = jnp.einsum("cbijk,bk->cbij", gathered, weights[2], precision=lax.Precision.HIGHEST)
        rs_plane = weights[0][:, :, None] * weights[1][:, None, :]
        return jnp.sum(along * rs_plane[None], axis=(2, 3))

    departed = lax.map(one_block, (coord_blocks, owner_blocks)).transpose(1, 0, 2)
    nodal_cube = departed.reshape(3, ELEMS, 8, 8, 8)
    own_faces = faces_of(nodal_cube)
    present = neighbours >= 0
    local_index = jnp.maximum(neighbours, 0).astype(jnp.int32)
    result = apply_faces(nodal_cube, own_faces, own_faces, local_index, present)
    return result.reshape(3, ELEMS, 512)
```

```python
import functools
import math

import jax
import jax.numpy as jnp
import numpy as np
from jax import lax
from jax.experimental import pallas as pl
from jax.experimental.pallas import tpu as pltpu
from jax.sharding import PartitionSpec as P

GLL_POINTS = np.array(
    [
        -1.0,
        -0.8717401485096066,
        -0.5917001814331423,
        -0.2092992179024789,
        0.2092992179024789,
        0.5917001814331423,
        0.8717401485096066,
        1.0,
    ]
)
ROW = 512
f32 = jnp.float32
bf16 = jnp.bfloat16


def split(values):
    head = values.astype(bf16)
    return head, (values - head.astype(f32)).astype(bf16)


def dot(lhs, rhs, dims):
    return lax.dot_general(lhs, rhs, (dims, ((), ())), preferred_element_type=f32)


def place_kernel(depart, owners, elems, placed, spots, acc, *, peers, width, rows_step):
    rows_all = placed.shape[1]
    capacity = rows_all // peers * width
    total = rows_step * ROW
    sub = 256
    before = lax.broadcasted_iota(jnp.int32, (sub, sub), 0) < lax.broadcasted_iota(
        jnp.int32, (sub, sub), 1
    )
    before = jnp.where(before, 1.0, 0.0).astype(bf16)
    peer_ids = lax.broadcasted_iota(jnp.int32, (peers, sub), 0)
    bucket_ids = lax.broadcasted_iota(jnp.int32, (rows_all, total), 0)
    place_ids = lax.broadcasted_iota(jnp.int32, (width, total), 0)
    acc[...] = jnp.zeros_like(acc)

    def add_step(step, count):
        first = step * rows_step
        owner_rows = [owners[pl.ds(first + row, 1), :] for row in range(rows_step)]
        pieces = [
            owner[:, at * sub : (at + 1) * sub] for owner in owner_rows for at in range(ROW // sub)
        ]
        hots = [jnp.where(peer_ids == piece, 1.0, 0.0) for piece in pieces]
        ranks = dot(jnp.concatenate(hots, axis=0).astype(bf16), before, ((1,), (0,)))
        spot_rows = []
        for at, hot in enumerate(hots):
            rank = ranks[at * peers : (at + 1) * peers]
            slot = jnp.sum(hot * (rank + count), axis=0, keepdims=True)
            spot_rows.append(pieces[at] * capacity + slot.astype(jnp.int32))
            count = count + jnp.sum(hot, axis=1, keepdims=True)
        spot = jnp.concatenate(spot_rows, axis=1)
        for row in range(rows_step):
            spots[pl.ds(first + row, 1), :] = spot[:, row * ROW : (row + 1) * ROW]
        bucket = spot // width
        bucket_hot = bucket_ids == bucket
        place_hot = jnp.where(place_ids == spot - bucket * width, 1.0, 0.0).astype(bf16)
        heads, tails = [], []
        for axis in range(3):
            value = jnp.concatenate(
                [depart[axis, pl.ds(first + row, 1), :] for row in range(rows_step)], axis=1
            )
            head = value.astype(bf16).astype(f32)
            heads.append(head)
            tails.append(value - head)
        elem = jnp.concatenate(
            [elems[pl.ds(first + row, 1), :] for row in range(rows_step)], axis=1
        )
        spread = [
            jnp.where(bucket_hot, value, 0.0).astype(bf16)
            for value in heads + tails + [elem.astype(f32)]
        ]
        acc[...] += dot(jnp.concatenate(spread, axis=0), place_hot, ((1,), (1,)))
        return count

    lax.fori_loop(0, owners.shape[0] // rows_step, add_step, jnp.zeros((peers, 1), f32))
    for axis in range(3):
        placed[axis] = (
            acc[axis * rows_all : (axis + 1) * rows_all]
            + acc[(3 + axis) * rows_all : (4 + axis) * rows_all]
        )
    placed[3] = acc[6 * rows_all : 7 * rows_all]


STEP = 8


def place(depart, owners, elems, peers, width):
    rows = depart.shape[1]
    rows_all = 2 * rows * ROW // width
    return pl.pallas_call(
        functools.partial(
            place_kernel, peers=peers, width=width, rows_step=math.gcd(rows, STEP)
        ),
        out_shape=[
            jax.ShapeDtypeStruct((4, rows_all, width), f32),
            jax.ShapeDtypeStruct((rows, ROW), jnp.int32),
        ],
        scratch_shapes=[pltpu.VMEM((7 * rows_all, width), f32)],
    )(depart, owners, elems)


def basis(coord):
    nodes = lax.broadcasted_iota(jnp.int32, (8, 1), 0)
    scale = jnp.zeros((8, 1), f32)
    for i in range(8):
        gaps = [GLL_POINTS[i] - GLL_POINTS[m] for m in range(8) if m != i]
        scale = jnp.where(nodes == i, float(1.0 / np.prod(gaps)), scale)
    spread = jnp.broadcast_to(coord, (8, coord.shape[1]))
    product = jnp.broadcast_to(scale, spread.shape)
    for m in range(8):
        product = product * jnp.where(nodes == m, 1.0, spread - float(GLL_POINTS[m]))
    return product


def interp_kernel(received, table, answers, parts, *, elem_count):
    @pl.when(pl.program_id(0) == 0)
    def _():
        parts[...] = jnp.concatenate(split(table[...]), axis=0)

    width = received.shape[2]
    elem_ids = lax.broadcasted_iota(jnp.int32, (elem_count, width), 0).astype(f32)
    both = parts[...]
    half = both.shape[0] // 2
    for row in range(received.shape[1]):
        weights = [basis(received[axis, row : row + 1, :]) for axis in range(3)]
        hot = elem_ids == received[3, row : row + 1, :]
        head = weights[2].astype(bf16).astype(f32)
        tail = weights[2] - head
        scaled_head = jnp.concatenate(
            [jnp.where(hot, head[k : k + 1], 0.0).astype(bf16) for k in range(8)], axis=0
        )
        scaled_tail = jnp.concatenate(
            [jnp.where(hot, tail[k : k + 1], 0.0).astype(bf16) for k in range(8)], axis=0
        )
        main = dot(both, scaled_head, ((1,), (0,)))
        rest = dot(both[:half], scaled_tail, ((1,), (0,)))
        along = main[:half] + main[half:] + rest
        for c in range(3):
            summed = along[c * 64 : c * 64 + 8] * weights[0][0:1]
            for i in range(1, 8):
                at = c * 64 + i * 8
                summed = summed + along[at : at + 8] * weights[0][i : i + 1]
            answers[c, row : row + 1, :] = jnp.sum(summed * weights[1], axis=0, keepdims=True)


def interpolate(received, table, elem_count):
    rows_all, width = received.shape[1:]
    rows_step = 8
    return pl.pallas_call(
        functools.partial(interp_kernel, elem_count=elem_count),
        grid=(rows_all // rows_step,),
        in_specs=[
            pl.BlockSpec((4, rows_step, width), lambda i: (0, i, 0)),
            pl.BlockSpec(table.shape, lambda i: (0, 0)),
        ],
        out_specs=pl.BlockSpec((3, rows_step, width), lambda i: (0, i, 0)),
        out_shape=jax.ShapeDtypeStruct((3, rows_all, width), f32),
        scratch_shapes=[pltpu.VMEM((2 * table.shape[0], table.shape[1]), bf16)],
        compiler_params=pltpu.CompilerParams(dimension_semantics=("arbitrary",)),
    )(received, table)


def pick_kernel(answers, spots, departed, parts):
    rows_all, width = answers.shape[1:]

    @pl.when(pl.program_id(0) == 0)
    def _():
        for c in range(3):
            head, tail = split(answers[c])
            parts[c * rows_all : (c + 1) * rows_all] = head
            parts[(3 + c) * rows_all : (4 + c) * rows_all] = tail

    for row in range(spots.shape[0]):
        spot = spots[row : row + 1, :]
        bucket = spot // width
        place_at = spot - bucket * width
        bucket_hot = lax.broadcasted_iota(jnp.int32, (rows_all, ROW), 0) == bucket
        place_hot = lax.broadcasted_iota(jnp.int32, (width, ROW), 0) == place_at
        place_hot = jnp.where(place_hot, 1.0, 0.0).astype(bf16)
        picked = dot(parts[...], place_hot, ((1,), (0,)))
        for c in range(3):
            both = (
                picked[c * rows_all : (c + 1) * rows_all]
                + picked[(3 + c) * rows_all : (4 + c) * rows_all]
            )
            departed[c, row : row + 1, :] = jnp.sum(
                jnp.where(bucket_hot, both, 0.0), axis=0, keepdims=True
            )


def pick(answers, spots):
    rows_all, width = answers.shape[1:]
    rows = spots.shape[0]
    rows_step = math.gcd(rows, 8)
    return pl.pallas_call(
        pick_kernel,
        grid=(rows // rows_step,),
        in_specs=[
            pl.BlockSpec((3, rows_all, width), lambda i: (0, 0, 0)),
            pl.BlockSpec((rows_step, ROW), lambda i: (i, 0)),
        ],
        out_specs=pl.BlockSpec((3, rows_step, ROW), lambda i: (0, i, 0)),
        out_shape=jax.ShapeDtypeStruct((3, rows, ROW), f32),
        scratch_shapes=[pltpu.VMEM((6 * rows_all, width), bf16)],
        compiler_params=pltpu.CompilerParams(dimension_semantics=("arbitrary",)),
    )(answers, spots)


def faces_kernel(own, before, after, across, advected, stacked):
    elem_count, nodes = own.shape[1:]
    extended = 3 * elem_count
    lanes = lax.broadcasted_iota(jnp.int32, (1, nodes), 1)
    columns = lax.broadcasted_iota(jnp.int32, (elem_count, extended), 1)
    pickers = []
    kept = jnp.ones((elem_count, nodes), f32)
    edges = []
    for face in range(6):
        stride = (64, 8, 1)[face // 2]
        edge = (lanes // stride) % 8 == 7 * (face % 2)
        edges.append(edge)
        there = across[:, face : face + 1]
        pickers.append(jnp.where(columns == there, 0.5, 0.0).astype(bf16))
        kept = kept - jnp.where(jnp.logical_and(edge, there >= 0), 0.5, 0.0)
    picker = jnp.concatenate(pickers, axis=1)
    for c in range(3):
        values = jnp.concatenate([before[c], own[c], after[c]], axis=0)
        for face in range(6):
            jump = 7 * (64, 8, 1)[face // 2]
            turn = jump if face % 2 else nodes - jump
            moved = jnp.where(edges[face], pltpu.roll(values, turn, 1), 0.0)
            head, tail = split(moved)
            stacked[face * extended : (face + 1) * extended, :nodes] = head
            stacked[face * extended : (face + 1) * extended, nodes:] = tail
        added = dot(picker, stacked[...], ((1,), (0,)))
        advected[c] = own[c] * kept + added[:, :nodes] + added[:, nodes:]


def faces(own, before, after, across):
    elem_count, nodes = own.shape[1:]
    return pl.pallas_call(
        faces_kernel,
        out_shape=jax.ShapeDtypeStruct(own.shape, f32),
        scratch_shapes=[pltpu.VMEM((18 * elem_count, 2 * nodes), bf16)],
    )(own, before, after, across)


def local(velocity, depart, owner_rank, owner_element_index, neighbours):
    axes = ("gx", "gy")
    inner_count = lax.axis_size("gy")
    peers = lax.axis_size("gx") * inner_count
    elem_count = velocity.shape[1]
    points = depart.shape[1]
    capacity = 2 * points // peers
    width = math.gcd(capacity, ROW)
    rows = points // ROW
    placed, spots = place(
        depart.reshape(3, rows, ROW),
        owner_rank.reshape(rows, ROW),
        owner_element_index.reshape(rows, ROW),
        peers,
        width,
    )
    table = (
        velocity.reshape(3, elem_count, 64, 8).transpose(0, 2, 3, 1).reshape(192, 8 * elem_count)
    )
    received = lax.all_to_all(placed, axes, split_axis=1, concat_axis=1, tiled=True)
    answers = interpolate(received, table, elem_count)
    answers = lax.all_to_all(answers, axes, split_axis=1, concat_axis=1, tiled=True)
    departed = pick(answers, spots).reshape(3, elem_count, 512)
    ends = peers - 1
    before = lax.ppermute(departed, axes, [(i, i + 1) for i in range(ends)])
    after = lax.ppermute(departed, axes, [(i + 1, i) for i in range(ends)])
    device_id = lax.axis_index("gx") * inner_count + lax.axis_index("gy")
    first_elem = (device_id - 1) * elem_count
    across = jnp.where(neighbours >= 0, neighbours - first_elem, -1).T
    return faces(departed, before, after, across)


def solution(mesh):
    placed = (
        P(None, ("gx", "gy"), None),
        P(None, ("gx", "gy")),
        P(("gx", "gy"), None),
        P(("gx", "gy")),
        P(None, ("gx", "gy")),
    )
    return jax.shard_map(
        local, mesh=mesh, in_specs=placed, out_specs=P(None, ("gx", "gy"), None), check_vma=False
    )
```

```python
import functools
import itertools
import math

import jax
import jax.numpy as jnp
import numpy as np
from jax import lax
from jax.experimental import pallas as pl
from jax.experimental.pallas import tpu as pltpu
from jax.sharding import PartitionSpec as P

GLL_POINTS = np.array(
    [
        -1.0,
        -0.8717401485096066,
        -0.5917001814331423,
        -0.2092992179024789,
        0.2092992179024789,
        0.5917001814331423,
        0.8717401485096066,
        1.0,
    ]
)
ROW = 512
f32 = jnp.float32
bf16 = jnp.bfloat16


def split(values):
    head = values.astype(bf16)
    return head, (values - head.astype(f32)).astype(bf16)


def dot(lhs, rhs, dims):
    return lax.dot_general(lhs, rhs, (dims, ((), ())), preferred_element_type=f32)


def place_kernel(depart, owners, elems, placed, spots, acc, *, peers, width, rows_step):
    capacity = placed.shape[1] // 4 * width
    rows_all = peers * capacity // width
    total = rows_step * ROW
    sub = 256
    before = lax.broadcasted_iota(jnp.int32, (sub, sub), 0) < lax.broadcasted_iota(
        jnp.int32, (sub, sub), 1
    )
    before = jnp.where(before, 1.0, 0.0).astype(bf16)
    peer_ids = lax.broadcasted_iota(jnp.int32, (peers, sub), 0)
    bucket_ids = lax.broadcasted_iota(jnp.int32, (rows_all, total), 0)
    place_ids = lax.broadcasted_iota(jnp.int32, (width, total), 0)
    acc[...] = jnp.zeros_like(acc)

    def add_step(step, count):
        first = step * rows_step
        lines = total // 128
        owner = owners[pl.ds(pl.multiple_of(step * lines, lines), lines), :]
        pieces = [
            jnp.concatenate([owner[at : at + 1], owner[at + 1 : at + 2]], axis=1)
            for at in range(0, lines, 2)
        ]
        hots = [jnp.where(peer_ids == piece, 1.0, 0.0) for piece in pieces]
        ranks = dot(jnp.concatenate(hots, axis=0).astype(bf16), before, ((1,), (0,)))
        spot_rows = []
        for at, hot in enumerate(hots):
            rank = ranks[at * peers : (at + 1) * peers]
            slot = jnp.sum(hot * (rank + count), axis=0, keepdims=True)
            spot_rows.append(pieces[at] * capacity + slot.astype(jnp.int32))
            count = count + jnp.sum(hot, axis=1, keepdims=True)
        spot = jnp.concatenate(spot_rows, axis=1)
        for row in range(rows_step):
            spots[pl.ds(first + row, 1), :] = spot[:, row * ROW : (row + 1) * ROW]
        bucket = spot // width
        bucket_hot = bucket_ids == bucket
        place_hot = jnp.where(place_ids == spot - bucket * width, 1.0, 0.0).astype(bf16)
        heads, tails = [], []
        for axis in range(3):
            value = depart[axis : axis + 1, pl.ds(pl.multiple_of(step * total, total), total)]
            head = value.astype(bf16).astype(f32)
            heads.append(head)
            tails.append(value - head)
        elem = elems[pl.ds(pl.multiple_of(step * lines, lines), lines), :]
        elem = jnp.concatenate([elem[at : at + 1] for at in range(lines)], axis=1)
        spread = [
            jnp.where(bucket_hot, value, 0.0).astype(bf16)
            for value in heads + [elem.astype(f32)] + tails
        ]
        acc[...] += dot(jnp.concatenate(spread, axis=0), place_hot, ((1,), (1,)))
        return count

    steps = owners.shape[0] * 128 // total
    lax.fori_loop(0, steps, add_step, jnp.zeros((peers, 1), f32))
    each = capacity // width
    for peer in range(peers):
        for channel in range(4):
            at = channel * rows_all + peer * each
            value = acc[at : at + each, :]
            if channel < 3:
                value = value + acc[at + 4 * rows_all : at + 4 * rows_all + each, :]
            placed[peer, channel * each : (channel + 1) * each, :] = value


STEP = 8


def place(depart, owners, elems, peers, width):
    points = depart.shape[1]
    rows = points // ROW
    rows_all = 2 * points // width
    return pl.pallas_call(
        functools.partial(
            place_kernel, peers=peers, width=width, rows_step=math.gcd(rows, STEP)
        ),
        out_shape=[
            jax.ShapeDtypeStruct((peers, 4 * rows_all // peers, width), f32),
            jax.ShapeDtypeStruct((rows, ROW), jnp.int32),
        ],
        scratch_shapes=[pltpu.VMEM((7 * rows_all, width), f32)],
    )(depart, owners, elems)


def basis(coord):
    nodes = lax.broadcasted_iota(jnp.int32, (8, 1), 0)
    scale = jnp.zeros((8, 1), f32)
    for i in range(8):
        gaps = [GLL_POINTS[i] - GLL_POINTS[m] for m in range(8) if m != i]
        scale = jnp.where(nodes == i, float(1.0 / np.prod(gaps)), scale)
    spread = jnp.broadcast_to(coord, (8, coord.shape[1]))
    product = jnp.broadcast_to(scale, spread.shape)
    for m in range(8):
        product = product * jnp.where(nodes == m, 1.0, spread - float(GLL_POINTS[m]))
    return product


def interp_kernel(received, table, answers, parts, *, elem_count):
    @pl.when(pl.program_id(0) == 0)
    def _():
        parts[...] = jnp.concatenate(split(table[...]), axis=0)

    width = received.shape[2]
    elem_ids = lax.broadcasted_iota(jnp.int32, (elem_count, width), 0).astype(f32)
    both = parts[...]
    half = both.shape[0] // 2
    each = received.shape[1] // 4
    for peer, row in itertools.product(range(received.shape[0]), range(each)):
        lines = [received[peer, c * each + row : c * each + row + 1, :] for c in range(4)]
        weights = [basis(lines[axis]) for axis in range(3)]
        hot = elem_ids == lines[3]
        head = weights[2].astype(bf16).astype(f32)
        tail = weights[2] - head
        scaled_head = jnp.concatenate(
            [jnp.where(hot, head[k : k + 1], 0.0).astype(bf16) for k in range(8)], axis=0
        )
        scaled_tail = jnp.concatenate(
            [jnp.where(hot, tail[k : k + 1], 0.0).astype(bf16) for k in range(8)], axis=0
        )
        main = dot(both, scaled_head, ((1,), (0,)))
        rest = dot(both[:half], scaled_tail, ((1,), (0,)))
        along = main[:half] + main[half:] + rest
        for c in range(3):
            summed = along[c * 64 : c * 64 + 8] * weights[0][0:1]
            for i in range(1, 8):
                at = c * 64 + i * 8
                summed = summed + along[at : at + 8] * weights[0][i : i + 1]
            value = jnp.sum(summed * weights[1], axis=0, keepdims=True)
            first = (c * each + row) * (width // 128)
            for at in range(width // 128):
                answers[peer, first + at : first + at + 1, :] = value[:, at * 128 : (at + 1) * 128]


def interpolate(received, table, elem_count):
    peers, channels, width = received.shape
    each = channels // 4
    peers_step = math.gcd(peers, max(1, 8 // each))
    lines = 3 * each * width // 128
    return pl.pallas_call(
        functools.partial(interp_kernel, elem_count=elem_count),
        grid=(peers // peers_step,),
        in_specs=[
            pl.BlockSpec((peers_step, channels, width), lambda i: (i, 0, 0)),
            pl.BlockSpec(table.shape, lambda i: (0, 0)),
        ],
        out_specs=pl.BlockSpec((peers_step, lines, 128), lambda i: (i, 0, 0)),
        out_shape=jax.ShapeDtypeStruct((peers, lines, 128), f32),
        scratch_shapes=[pltpu.VMEM((2 * table.shape[0], table.shape[1]), bf16)],
        compiler_params=pltpu.CompilerParams(dimension_semantics=("arbitrary",)),
    )(received, table)


def pick_kernel(answers, spots, departed, gathered, parts):
    width = parts.shape[1]
    rows_all = parts.shape[0] // 6
    each = rows_all // answers.shape[0]
    pieces = width // 128

    @pl.when(pl.program_id(0) == 0)
    def _():
        for peer, c, row, at in itertools.product(
            range(answers.shape[0]), range(3), range(each), range(pieces)
        ):
            line = (c * each + row) * pieces + at
            into = c * rows_all + peer * each + row
            gathered[into : into + 1, at * 128 : (at + 1) * 128] = answers[
                peer, line : line + 1, :
            ]
        head, tail = split(gathered[...])
        parts[: 3 * rows_all] = head
        parts[3 * rows_all :] = tail

    for row in range(spots.shape[0]):
        spot = spots[row : row + 1, :]
        bucket = spot // width
        place_at = spot - bucket * width
        bucket_hot = lax.broadcasted_iota(jnp.int32, (rows_all, ROW), 0) == bucket
        place_hot = lax.broadcasted_iota(jnp.int32, (width, ROW), 0) == place_at
        place_hot = jnp.where(place_hot, 1.0, 0.0).astype(bf16)
        picked = dot(parts[...], place_hot, ((1,), (0,)))
        for c in range(3):
            both = (
                picked[c * rows_all : (c + 1) * rows_all]
                + picked[(3 + c) * rows_all : (4 + c) * rows_all]
            )
            departed[c, row : row + 1, :] = jnp.sum(
                jnp.where(bucket_hot, both, 0.0), axis=0, keepdims=True
            )


def pick(answers, spots, width):
    peers, lines, _ = answers.shape
    rows_all = peers * lines * 128 // (3 * width)
    rows = spots.shape[0]
    rows_step = math.gcd(rows, 8)
    return pl.pallas_call(
        pick_kernel,
        grid=(rows // rows_step,),
        in_specs=[
            pl.BlockSpec(answers.shape, lambda i: (0, 0, 0)),
            pl.BlockSpec((rows_step, ROW), lambda i: (i, 0)),
        ],
        out_specs=pl.BlockSpec((3, rows_step, ROW), lambda i: (0, i, 0)),
        out_shape=jax.ShapeDtypeStruct((3, rows, ROW), f32),
        scratch_shapes=[
            pltpu.VMEM((3 * rows_all, width), f32),
            pltpu.VMEM((6 * rows_all, width), bf16),
        ],
        compiler_params=pltpu.CompilerParams(dimension_semantics=("arbitrary",)),
    )(answers, spots)


def faces_kernel(own, before, after, across, advected, stacked):
    elem_count, nodes = own.shape[1:]
    extended = 3 * elem_count
    lanes = lax.broadcasted_iota(jnp.int32, (1, nodes), 1)
    columns = lax.broadcasted_iota(jnp.int32, (elem_count, extended), 1)
    pickers = []
    kept = jnp.ones((elem_count, nodes), f32)
    edges = []
    for face in range(6):
        stride = (64, 8, 1)[face // 2]
        edge = (lanes // stride) % 8 == 7 * (face % 2)
        edges.append(edge)
        there = across[:, face : face + 1]
        pickers.append(jnp.where(columns == there, 0.5, 0.0).astype(bf16))
        kept = kept - jnp.where(jnp.logical_and(edge, there >= 0), 0.5, 0.0)
    picker = jnp.concatenate(pickers, axis=1)
    for c in range(3):
        values = jnp.concatenate([before[c], own[c], after[c]], axis=0)
        for face in range(6):
            jump = 7 * (64, 8, 1)[face // 2]
            turn = jump if face % 2 else nodes - jump
            moved = jnp.where(edges[face], pltpu.roll(values, turn, 1), 0.0)
            head, tail = split(moved)
            stacked[face * extended : (face + 1) * extended, :nodes] = head
            stacked[face * extended : (face + 1) * extended, nodes:] = tail
        added = dot(picker, stacked[...], ((1,), (0,)))
        advected[c] = own[c] * kept + added[:, :nodes] + added[:, nodes:]


def faces(own, before, after, across):
    elem_count, nodes = own.shape[1:]
    return pl.pallas_call(
        faces_kernel,
        out_shape=jax.ShapeDtypeStruct(own.shape, f32),
        scratch_shapes=[pltpu.VMEM((18 * elem_count, 2 * nodes), bf16)],
    )(own, before, after, across)


def local(velocity, depart, owner_rank, owner_element_index, neighbours):
    axes = ("gx", "gy")
    inner_count = lax.axis_size("gy")
    peers = lax.axis_size("gx") * inner_count
    elem_count = velocity.shape[1]
    points = depart.shape[1]
    capacity = 2 * points // peers
    width = math.gcd(capacity, ROW)
    placed, spots = place(
        depart,
        owner_rank.reshape(points // 128, 128),
        owner_element_index.reshape(points // 128, 128),
        peers,
        width,
    )
    table = (
        velocity.reshape(3, elem_count, 64, 8).transpose(0, 2, 3, 1).reshape(192, 8 * elem_count)
    )
    received = lax.all_to_all(placed, axes, split_axis=0, concat_axis=0, tiled=True)
    answers = interpolate(received, table, elem_count)
    answers = lax.all_to_all(answers, axes, split_axis=0, concat_axis=0, tiled=True)
    departed = pick(answers, spots, width).reshape(3, elem_count, 512)
    ends = peers - 1
    before = lax.ppermute(departed, axes, [(i, i + 1) for i in range(ends)])
    after = lax.ppermute(departed, axes, [(i + 1, i) for i in range(ends)])
    device_id = lax.axis_index("gx") * inner_count + lax.axis_index("gy")
    first_elem = (device_id - 1) * elem_count
    across = jnp.where(neighbours >= 0, neighbours - first_elem, -1).T
    return faces(departed, before, after, across)


def solution(mesh):
    placed = (
        P(None, ("gx", "gy"), None),
        P(None, ("gx", "gy")),
        P(("gx", "gy"), None),
        P(("gx", "gy")),
        P(None, ("gx", "gy")),
    )
    return jax.shard_map(
        local, mesh=mesh, in_specs=placed, out_specs=P(None, ("gx", "gy"), None), check_vma=False
    )
```
